32 devices in a mesh: groups: 2 (over x), seq: 8 (over z, y), head: 2 (over core).
Axes of the slice: x: 2, y: 2, z: 4, core: 2. Of those that a mesh axis runs over, the one named last changes fastest.
Arguments:
- queries: bfloat16 [2048, 28, 128], P(('groups', 'seq'), 'head'), parts along dimension 0, may hold values from -400 to 400, as said below
- request_image: int32 [2048, 1], P(('groups', 'seq')), parts along dimension 0, may hold values from 0 to 15; in each aligned block of 128 rows (0 to 127, 128 to 255, ...) at most 16 rows name the same one
- image_slot: int32 [32], P('groups'), parts along dimension 0, may hold values from 0 to 15, each once
- image_lengths: int32 [32], P(('groups', 'seq')), parts along dimension 0, may hold values from 640 to 1280
- image_keys: bfloat16 [32, 4, 1280, 128], P(('groups', 'seq'), 'head'), parts along dimension 0, may hold values from -6 to 6
- image_values: bfloat16 [32, 4, 1280, 128], P(('groups', 'seq'), 'head'), parts along dimension 0, may hold values from -6 to 6
- text_keys: bfloat16 [2048, 4, 64, 128], P(('groups', 'seq'), 'head'), parts along dimension 0, may hold values from -6 to 6
- text_values: bfloat16 [2048, 4, 64, 128], P(('groups', 'seq'), 'head'), parts along dimension 0, may hold values from -6 to 6
- text_lengths: int32 [2048], P(('groups', 'seq')), parts along dimension 0, may hold values from 1 to 64
Outputs:
- attention: bfloat16 [2048, 28, 128], P(('groups', 'seq'), 'head'), parts along dimension 0
The draws below stay inside these ranges and needn't reach their ends.
There are 2 independent parts, one for each index of `groups`. The reference program is written for one: setup_inputs(seed, part) draws one part's arguments, and reference() takes and returns one part's arrays. A program takes and returns all parts, laid end to end along the dimension named above; each array names one. Nothing has to cross between parts.
Inputs may be any that keep to these rules, and one draw needn't show every extreme that they name: queries are finite bfloat16 values. `request_image`: the requests of one index of seq name any one image at most 16 times, and in some index of seq some image is named exactly 16 times. `image_slot`: a permutation; the image in storage slot s is held by index s // 2 of seq.
All inputs are finite; a program needn't handle non-finite values.
Results may differ from the reference program's by a relative error of at most 0.0056.
Values may be sent and summed in bfloat16 or wider, within the bound.
A program may use at most 64 MiB of HBM per device.

```python
import math
import jax
import jax.numpy as jnp
import numpy as np
from jax import lax

D_HEAD = 128
KV_HEADS = 4
Q_HEADS = 28
IMG_TOK = 1280
TXT_TOK = 64
REQ_DEV = 128
REQUESTS = 1024
IMAGES = 16
MOST = 16


def draw_queries(key, part):
    base = jax.random.truncated_normal(key, -6.0, 6.0, (REQUESTS, Q_HEADS, D_HEAD), jnp.float32)
    return base.astype(jnp.bfloat16)


def touch_ends(drawn, own_key, smallest, high):
    spot = [jax.random.randint(jax.random.fold_in(own_key, axis), (), 0, length) for axis, length in enumerate(drawn.shape)]
    longest = drawn.shape.index(max(drawn.shape))
    neighbour = spot[:longest] + [(spot[longest] + 1) % drawn.shape[longest]] + spot[longest + 1:]
    return drawn.at[tuple(spot)].set(smallest).at[tuple(neighbour)].set(high)


def level_of(rng, extent, shards, smallest, largest):
    level, own = 1.0, jax.random.fold_in(rng, 6)
    for axis_at, shards_of in shards:
        steps = jnp.exp(jax.random.uniform(jax.random.fold_in(own, axis_at), (shards_of,), jnp.float32, smallest / len(shards), largest / len(shards)))
        level = level * jnp.repeat(steps, extent[axis_at] // shards_of).reshape([-1 if axis == axis_at else 1 for axis in range(len(extent))])
    return level


def routed_block(rng, own, number, rows, amount, top, limit, slope):
    ranking = jax.random.permutation(rng, amount)
    crowded, ordinary = portions_of(amount, rows * top, limit, slope, True), portions_of(amount, rows * top, limit, slope, False)
    places = jnp.arange(amount)

    def named(lengths, rotation):
        used = int((lengths > 0).sum())
        fixed = max(1, used // 4)
        passed = fixed + (places - fixed + rotation * (used - fixed)) % max(1, amount - fixed)
        return jnp.zeros((amount,), jnp.int32).at[ranking[jnp.where(places < fixed, places, passed)]].set(jnp.asarray(lengths, jnp.int32))

    lengths = jnp.where(number % 4 == 0, named(crowded, number // 4), named(ordinary, number - number // 4 - 1))
    mixed = jax.random.permutation(jax.random.fold_in(own, 3), amount)
    source_of, receiver = mixed[0:amount // 2 * 2:2], mixed[1:amount // 2 * 2:2]
    slack = jnp.minimum(lengths[source_of] - 1, limit - lengths[receiver]) // 2
    slack = jnp.where((source_of == ranking[0]) | (receiver == ranking[0]) | (lengths[receiver] == 0), 0, jnp.maximum(slack, 0))
    passed = jax.random.randint(jax.random.fold_in(own, 4), (amount // 2,), 0, 1 << 20) % (slack + 1)
    lengths = lengths.at[source_of].add(-passed).at[receiver].add(passed)
    members = jnp.searchsorted(jnp.cumsum(lengths), jnp.arange(rows * top), side="right").astype(jnp.int32)
    grid = members.reshape(top, rows).T
    grid = grid[jax.random.permutation(jax.random.fold_in(own, 1), rows)]
    rotation = jax.random.randint(jax.random.fold_in(own, 2), (rows, 1), 0, top)
    return jnp.take_along_axis(grid, (jnp.arange(top)[None, :] + rotation) % top, axis=1)


def portions_of(number_of, total, reach, slope, full):
    weights = [(1 << 20) // math.isqrt(grade ** slope) + 1 for grade in range(1, number_of + 1)]
    largest = reach if full else min(reach, max(-(-total // number_of), total * weights[0] // sum(weights)))
    least = 1 if total - largest >= number_of - 1 else 0
    given, spare = [largest] + [least] * (number_of - 1), total - largest - least * (number_of - 1)
    while spare > 0:
        candidates = [i for i in range(1, number_of) if given[i] < largest] or [i for i in range(1, number_of) if given[i] < reach]
        whole, remaining = sum([weights[i] for i in candidates]), spare
        for i in candidates:
            extra = min(reach - given[i], max(1, remaining * weights[i] // whole), spare)
            given[i] = given[i] + extra
            spare = spare - extra
    return np.array(given)


def scatter_about(key, extent, deviation, reach, split=(), held_as=jnp.bfloat16):
    result = deviation * jax.random.normal(key, extent, jnp.float32)
    if split:
        result = result * level_of(key, extent, split, -0.22, 0.18)
    return jnp.clip(result, -reach, reach).astype(held_as)


def setup_inputs(seed: int = 0, part: int = 0) -> dict:
    key_of = jax.random.split(jax.random.key(seed), 10)
    part_splits = jax.random.split(jax.random.fold_in(key_of[9], part), 10)
    queries = draw_queries(jax.random.fold_in(jax.random.fold_in(key_of[9], part), 71), part)
    request_image_keys = jax.random.split(jax.random.fold_in(part_splits[1], 1), REQUESTS // REQ_DEV)
    request_image_turns = jax.random.permutation(jax.random.fold_in(part_splits[1], 3), REQUESTS // REQ_DEV)
    request_image = jax.vmap(lambda own, number: routed_block(jax.random.fold_in(part_splits[1], 2), own, number, REQ_DEV, IMAGES, 1, MOST, 2))(request_image_keys, request_image_turns).reshape((REQUESTS, 1))
    image_slot = jax.random.permutation(part_splits[2], IMAGES).astype(jnp.int32)
    image_lengths = touch_ends(jax.random.randint(part_splits[3], (IMAGES,), IMG_TOK // 2, IMG_TOK + 1), jax.random.fold_in(part_splits[3], 1), IMG_TOK // 2, IMG_TOK).astype(jnp.int32)
    image_keys = scatter_about(part_splits[4], (IMAGES, KV_HEADS, IMG_TOK, D_HEAD), 1.0, 6.0, ((0, 8), (1, 2)))
    image_values = scatter_about(part_splits[5], (IMAGES, KV_HEADS, IMG_TOK, D_HEAD), 1.0, 6.0, ((0, 8), (1, 2)))
    text_keys = scatter_about(part_splits[6], (REQUESTS, KV_HEADS, TXT_TOK, D_HEAD), 1.0, 6.0, ((0, 8), (1, 2)))
    text_values = scatter_about(part_splits[7], (REQUESTS, KV_HEADS, TXT_TOK, D_HEAD), 1.0, 6.0, ((0, 8), (1, 2)))
    text_lengths = touch_ends(jax.random.randint(part_splits[8], (REQUESTS,), 1, TXT_TOK + 1), jax.random.fold_in(part_splits[8], 1), 1, TXT_TOK).astype(jnp.int32)
    return dict(queries=queries, request_image=request_image, image_slot=image_slot, image_lengths=image_lengths, image_keys=image_keys, image_values=image_values, text_keys=text_keys, text_values=text_values, text_lengths=text_lengths)


NEGATIVE = -1e+30

def partial_attend(query_heads, keys, values, valid, scale):
    scores = jnp.einsum('bhgd,bhtd->bhgt', query_heads, keys) * scale
    scores = jnp.where(valid, scores, NEGATIVE)
    highest = lax.optimization_barrier(jnp.max(scores, axis=-1, keepdims=True))
    weights = jnp.where(valid, jnp.exp(scores - highest), 0.0)
    total = lax.optimization_barrier(jnp.sum(weights, axis=-1, keepdims=True))
    rounded = lax.optimization_barrier(weights.astype(jnp.bfloat16)).astype(jnp.float32)
    output = jnp.einsum('bhgt,bhtd->bhgd', rounded, values) / total
    return (output, highest[..., 0] + jnp.log(total[..., 0]))

def merge_parts(image_out, image_lse, text_out, text_lse):
    highest = jnp.maximum(image_lse, text_lse)
    image_weight = jnp.exp(image_lse - highest)[..., None]
    text_weight = jnp.exp(text_lse - highest)[..., None]
    return (image_weight * image_out + text_weight * text_out) / (image_weight + text_weight)

def reference(queries, request_image, image_slot, image_lengths, image_keys, image_values, text_keys, text_values, text_lengths):
    scale = 1.0 / math.sqrt(D_HEAD)
    group = Q_HEADS // KV_HEADS
    slots = image_slot[request_image[:, 0]].astype(jnp.int32)
    blocks = REQUESTS // REQ_DEV

    def one_block(packed):
        block_queries, block_slots, block_tkeys, block_tvalues, block_tlen = packed
        query_heads = block_queries.astype(jnp.float32).reshape(REQ_DEV, KV_HEADS, group, D_HEAD)
        keys = image_keys[block_slots].astype(jnp.float32)
        values = image_values[block_slots].astype(jnp.float32)
        image_valid = (jnp.arange(IMG_TOK, dtype=jnp.int32)[None, :] < image_lengths[block_slots][:, None])[:, None, None, :]
        image_out, image_lse = partial_attend(query_heads, keys, values, image_valid, scale)
        image_out = lax.optimization_barrier(image_out.astype(jnp.bfloat16)).astype(jnp.float32)
        text_valid = (jnp.arange(TXT_TOK, dtype=jnp.int32)[None, :] < block_tlen[:, None])[:, None, None, :]
        text_out, text_lse = partial_attend(query_heads, block_tkeys.astype(jnp.float32), block_tvalues.astype(jnp.float32), text_valid, scale)
        merged = merge_parts(image_out, image_lse, text_out, text_lse)
        return merged.reshape(REQ_DEV, Q_HEADS, D_HEAD).astype(jnp.bfloat16)
    packed = (queries.reshape(blocks, REQ_DEV, Q_HEADS, D_HEAD), slots.reshape(blocks, REQ_DEV), text_keys.reshape(blocks, REQ_DEV, KV_HEADS, TXT_TOK, D_HEAD), text_values.reshape(blocks, REQ_DEV, KV_HEADS, TXT_TOK, D_HEAD), text_lengths.reshape(blocks, REQ_DEV))
    return lax.map(one_block, packed).reshape(REQUESTS, Q_HEADS, D_HEAD)
```

```python
import functools
import math

import jax
import jax.numpy as jnp
from jax import lax
from jax.experimental import pallas as pl
from jax.experimental.pallas import tpu as pltpu
from jax.sharding import PartitionSpec as P

NEGATIVE = -1e30
LOG2E = math.log2(math.e)
LN2 = math.log(2.0)
MESH = pl.DeviceIdType.MESH
BLOCK = 16
LANES = 16
SPLIT = 3
FIRST = 1
LIMIT = 48 * 1024 * 1024


def partner(me, step, devices):
    other = 0
    bit = 1
    while bit < devices:
        mine = lax.rem(me // bit, 2)
        flip = lax.rem(step // bit, 2)
        other = other + bit * (mine + flip - 2 * mine * flip)
        bit *= 2
    return other


def attend(query, keys, values, mask, factor):
    scores = lax.dot_general(
        query, keys, (((1,), (1,)), ((), ())), preferred_element_type=jnp.float32
    )
    scores = mask(scores * factor)
    highest = jnp.max(scores, axis=-1, keepdims=True)
    weights = jnp.exp2(scores - highest)
    total = jnp.sum(weights, axis=-1, keepdims=True)
    output = jnp.dot(weights.astype(jnp.bfloat16), values, preferred_element_type=jnp.float32)
    return output / total, (highest + jnp.log2(total)) * LN2


def kernel(
    devices,
    held,
    most,
    group,
    slot_hbm,
    length_hbm,
    image_hbm,
    text_length_hbm,
    query_hbm,
    ikey_hbm,
    ivalue_hbm,
    tkey_hbm,
    tvalue_hbm,
    out_ref,
    slot_ref,
    length_ref,
    image_ref,
    text_length_ref,
    query_ref,
    ikey,
    ivalue,
    tkey,
    tvalue,
    send,
    recv,
    result,
    back,
    text_out,
    text_lse,
    lengths,
    local_sem,
    send_sem,
    recv_sem,
    result_sem,
    back_sem,
):
    me = lax.axis_index("seq")
    local_heads, rows, head_size = query_ref.shape
    local_kv = ikey.shape[1]
    image_tokens = ikey.shape[2]
    text_tokens = tkey.shape[2]
    images = slot_ref.shape[0]
    slots = images * most
    blocks = rows // BLOCK
    factor = LOG2E / math.sqrt(head_size)

    barrier = pltpu.get_barrier_semaphore()

    @pl.loop(1, devices)
    def _(step):
        pl.semaphore_signal(
            barrier, inc=1, device_id={"seq": partner(me, step, devices)}, device_id_type=MESH
        )

    copies = [
        pltpu.make_async_copy(source, target, local_sem.at[index])
        for index, (source, target) in enumerate(
            (
                (query_hbm, query_ref),
                (slot_hbm, slot_ref),
                (image_hbm, image_ref),
                (length_hbm, length_ref),
                (text_length_hbm, text_length_ref),
                (tkey_hbm, tkey),
                (tvalue_hbm, tvalue),
                (ikey_hbm, ikey),
                (ivalue_hbm, ivalue),
            )
        )
    ]
    for copy in copies:
        copy.start()
    loads = copies[5:]

    copies[1].wait()
    copies[2].wait()
    image = image_ref[...]
    slot = jnp.zeros_like(image)
    for index in range(images):
        place = slot_ref[index]
        place = partner(me, place // held, devices) * held + lax.rem(place, held)
        slot = jnp.where(image == index, place, slot)
    hits = slot == lax.broadcasted_iota(jnp.int32, (images, rows), 0)
    earlier = lax.broadcasted_iota(jnp.int32, (rows, rows), 0) < lax.broadcasted_iota(
        jnp.int32, (rows, rows), 1
    )
    counts = jnp.dot(
        hits.astype(jnp.float32).astype(jnp.bfloat16),
        earlier.astype(jnp.float32).astype(jnp.bfloat16),
        preferred_element_type=jnp.float32,
    )
    rank = jnp.sum(jnp.where(hits, counts, 0.0), axis=0, keepdims=True)
    target = slot.astype(jnp.float32) * most + rank
    dispatch = (
        lax.broadcasted_iota(jnp.int32, (slots, rows), 0).astype(jnp.float32) == target
    ).astype(jnp.float32).astype(jnp.bfloat16)
    copies[0].wait()
    for head in range(local_heads):
        moved = jnp.dot(dispatch, query_ref[head], preferred_element_type=jnp.float32)
        send[:, :, head] = moved.astype(jnp.bfloat16).reshape(devices, held, most, head_size)

    pl.semaphore_wait(barrier, devices - 1)

    def forward(step):
        return pltpu.make_async_remote_copy(
            src_ref=send.at[step],
            dst_ref=recv.at[step],
            send_sem=send_sem.at[step],
            recv_sem=recv_sem.at[step],
            device_id={"seq": partner(me, step, devices)},
            device_id_type=MESH,
        )

    def returning(step):
        return pltpu.make_async_remote_copy(
            src_ref=result.at[step],
            dst_ref=back.at[step],
            send_sem=result_sem.at[step],
            recv_sem=back_sem.at[step],
            device_id={"seq": partner(me, step, devices)},
            device_id_type=MESH,
        )

    @pl.loop(1, devices)
    def _(step):
        forward(step).start()

    copies[3].wait()
    copies[4].wait()
    lengths[...] = jnp.broadcast_to(
        text_length_ref[...].astype(jnp.float32), (rows, rows)
    ).T

    def place(lse, count):
        lane = lax.broadcasted_iota(jnp.int32, (count, head_size), 1)
        plane = jnp.zeros((count, head_size), jnp.float32)
        for head in range(local_heads):
            plane = jnp.where(lane == head, lse[head], plane)
        return plane

    loads[0].wait()
    loads[1].wait()

    def text(block):
        first = block * BLOCK
        first = first if isinstance(first, int) else pl.multiple_of(first, BLOCK)
        window = pl.ds(first, BLOCK)
        token = lax.broadcasted_iota(jnp.int32, (BLOCK, BLOCK * text_tokens), 1)
        offset = (
            token - text_tokens * lax.broadcasted_iota(jnp.int32, token.shape, 0)
        ).astype(jnp.float32)
        valid = (offset >= 0.0) & (offset < lengths[window, 0:1])
        bias = jnp.where(valid, 0.0, NEGATIVE)
        lses = []
        for kv in range(local_kv):
            query = query_ref[kv * group : (kv + 1) * group, window, :]
            query = query.reshape(group * BLOCK, head_size)
            keys = tkey[window, kv].reshape(BLOCK * text_tokens, head_size)
            values = tvalue[window, kv].reshape(BLOCK * text_tokens, head_size)

            def mask(scores):
                scores = scores.reshape(group, BLOCK, BLOCK * text_tokens) + bias[None]
                return scores.reshape(group * BLOCK, BLOCK * text_tokens)

            output, lse = attend(query, keys, values, mask, factor)
            text_out[kv * group : (kv + 1) * group, window, :] = output.reshape(
                group, BLOCK, head_size
            )
            lses += [lse[head * BLOCK : (head + 1) * BLOCK] for head in range(group)]
        text_lse[window, :] = place(lses, BLOCK)

    loads[2].wait()
    loads[3].wait()
    token = lax.broadcasted_iota(jnp.int32, (1, image_tokens), 1)
    biases = [jnp.where(token < length_ref[index], 0.0, NEGATIVE) for index in range(held)]

    def process(source, target):
        packed = jnp.zeros((most, head_size), jnp.float32)
        for index in range(held):
            lses = []
            for kv in range(local_kv):
                query = source[index, kv * group : (kv + 1) * group]
                query = query.reshape(group * most, head_size)
                output, lse = attend(
                    query,
                    ikey[index, kv],
                    ivalue[index, kv],
                    lambda scores: scores + biases[index],
                    factor,
                )
                start = index * local_heads + kv * group
                target[start : start + group] = output.astype(
                    jnp.bfloat16
                ).reshape(group, most, head_size)
                lses += [lse[head * most : (head + 1) * most] for head in range(group)]
            plane = place(lses, most)
            high = plane.astype(jnp.bfloat16).astype(jnp.float32)
            rest = plane - high
            middle = rest.astype(jnp.bfloat16).astype(jnp.float32)
            low = rest - middle
            for part, piece in enumerate((high, middle, low)):
                shift = LANES * (SPLIT * index + part)
                packed = packed + (pltpu.roll(piece, shift, 1) if shift else piece)
        target[held * local_heads] = packed.astype(jnp.bfloat16)

    for block in range(FIRST):
        text(block)
    process(send.at[0], back.at[0])

    @pl.loop(1, devices)
    def _(step):
        @pl.when(step + (FIRST - 1) < blocks)
        def _():
            text(step + (FIRST - 1))

        forward(step).wait_recv()
        process(recv.at[step], result.at[step])
        returning(step).start()

    for block in range(devices + FIRST - 1, blocks):
        text(block)

    sought = jnp.broadcast_to(target, (rows, rows)).T
    lane = lax.broadcasted_iota(jnp.int32, (rows, rows), 1).astype(jnp.float32)
    combine = jnp.concatenate(
        [
            (sought == lane + float(start)).astype(jnp.float32).astype(jnp.bfloat16)
            for start in range(0, slots, rows)
        ],
        axis=1,
    )

    @pl.loop(1, devices)
    def _(step):
        forward(step).wait_send()
        returning(step).wait_send()
        returning(step).wait_recv()

    planes = back[:, held * local_heads].reshape(devices, 1, most, head_size)
    spread = jnp.broadcast_to(planes, (devices, held, most, head_size)).reshape(slots, head_size)
    at_lane = lax.broadcasted_iota(jnp.int32, (1, 1, 1, head_size), 3)
    at_held = lax.broadcasted_iota(jnp.int32, (1, held, 1, 1), 1)
    low_lane = at_held * (SPLIT * LANES)
    own_lanes = (at_lane >= low_lane) & (at_lane < low_lane + SPLIT * LANES)
    own_lanes = jnp.broadcast_to(
        own_lanes.astype(jnp.float32), (devices, held, most, head_size)
    ).reshape(slots, head_size).astype(jnp.bfloat16)
    parts = jnp.dot(combine, spread * own_lanes, preferred_element_type=jnp.float32)
    image_lse = parts
    for piece in range(1, SPLIT * held):
        image_lse = image_lse + pltpu.roll(parts, head_size - LANES * piece, 1)
    own_lse = text_lse[...]
    upper = jnp.maximum(image_lse, own_lse)
    image_weight = jnp.exp(image_lse - upper)
    text_weight = jnp.exp(own_lse - upper)
    whole = image_weight + text_weight
    image_weight = image_weight / whole
    text_weight = text_weight / whole
    def gathered(head):
        pieces = [back[:, index * local_heads + head] for index in range(held)]
        return jnp.stack(pieces, axis=1).reshape(slots, head_size)

    for head in range(local_heads):
        image_part = jnp.dot(
            combine,
            gathered(head),
            preferred_element_type=jnp.float32,
        )
        merged = (
            image_weight[:, head : head + 1] * image_part
            + text_weight[:, head : head + 1] * text_out[head]
        )
        out_ref[head] = merged.astype(jnp.bfloat16)


def on_device(
    queries,
    request_image,
    image_slot,
    image_lengths,
    image_keys,
    image_values,
    text_keys,
    text_values,
    text_lengths,
):
    rows, local_heads, head_size = queries.shape
    held, local_kv, image_tokens, _ = image_keys.shape
    text_tokens = text_keys.shape[2]
    group = local_heads // local_kv
    images = image_slot.shape[0]
    devices = lax.axis_size("seq")
    most = -(-max(2, 2 * rows // images) // BLOCK) * BLOCK
    hbm = pl.BlockSpec(memory_space=pltpu.HBM)
    moved = pl.pallas_call(
        functools.partial(kernel, devices, held, most, group),
        out_shape=pltpu.VMEM((local_heads, rows, head_size), jnp.bfloat16),
        in_specs=[hbm] * 9,
        out_specs=pl.BlockSpec(memory_space=pltpu.VMEM),
        scratch_shapes=[
            pltpu.SMEM(image_slot.shape, jnp.int32),
            pltpu.SMEM(image_lengths.shape, jnp.int32),
            pltpu.VMEM((1, rows), jnp.int32),
            pltpu.VMEM((1, rows), jnp.int32),
            pltpu.VMEM((local_heads, rows, head_size), jnp.bfloat16),
            pltpu.VMEM(image_keys.shape, jnp.bfloat16),
            pltpu.VMEM(image_values.shape, jnp.bfloat16),
            pltpu.VMEM(text_keys.shape, jnp.bfloat16),
            pltpu.VMEM(text_values.shape, jnp.bfloat16),
            pltpu.VMEM((devices, held, local_heads, most, head_size), jnp.bfloat16),
            pltpu.VMEM((devices, held, local_heads, most, head_size), jnp.bfloat16),
            pltpu.VMEM((devices, held * local_heads + 1, most, head_size), jnp.bfloat16),
            pltpu.VMEM((devices, held * local_heads + 1, most, head_size), jnp.bfloat16),
            pltpu.VMEM((local_heads, rows, head_size), jnp.float32),
            pltpu.VMEM((rows, head_size), jnp.float32),
            pltpu.VMEM((rows, rows), jnp.float32),
            pltpu.SemaphoreType.DMA((9,)),
            pltpu.SemaphoreType.DMA((devices,)),
            pltpu.SemaphoreType.DMA((devices,)),
            pltpu.SemaphoreType.DMA((devices,)),
            pltpu.SemaphoreType.DMA((devices,)),
        ],
        compiler_params=pltpu.CompilerParams(
            collective_id=0, has_side_effects=True, vmem_limit_bytes=LIMIT
        ),
    )(
        *(
            pltpu.with_memory_space_constraint(operand, pltpu.HBM)
            for operand in (
                image_slot,
                image_lengths,
                request_image.reshape(1, rows),
                text_lengths.reshape(1, rows),
                jnp.transpose(queries, (1, 0, 2)),
                image_keys,
                image_values,
                text_keys,
                text_values,
            )
        )
    )
    return jnp.transpose(moved, (1, 0, 2))


def solution(mesh):
    in_specs = (
        P(("groups", "seq"), "head", None),
        P(("groups", "seq"), None),
        P("groups"),
        P(("groups", "seq")),
        P(("groups", "seq"), "head", None, None),
        P(("groups", "seq"), "head", None, None),
        P(("groups", "seq"), "head", None, None),
        P(("groups", "seq"), "head", None, None),
        P(("groups", "seq")),
    )
    out_specs = P(("groups", "seq"), "head", None)
    return jax.shard_map(
        on_device, mesh=mesh, in_specs=in_specs, out_specs=out_specs, check_vma=False
    )
```

```python
import functools
import math

import jax
import jax.numpy as jnp
from jax import lax
from jax.experimental import pallas as pl
from jax.experimental.pallas import tpu as pltpu
from jax.sharding import PartitionSpec as P

NEGATIVE = -1e30
LOG2E = math.log2(math.e)
LN2 = math.log(2.0)
MESH = pl.DeviceIdType.MESH
BLOCK = 16
LANES = 16
SPLIT = 3
FIRST = 1
LIMIT = 48 * 1024 * 1024


def partner(me, step, devices):
    other = 0
    bit = 1
    while bit < devices:
        mine = lax.rem(me // bit, 2)
        flip = lax.rem(step // bit, 2)
        other = other + bit * (mine + flip - 2 * mine * flip)
        bit *= 2
    return other


def attend(query, keys, values, mask, factor):
    scores = lax.dot_general(
        query, keys, (((1,), (1,)), ((), ())), preferred_element_type=jnp.float32
    )
    scores = mask(scores * factor)
    highest = jnp.max(scores, axis=-1, keepdims=True)
    weights = jnp.exp2(scores - highest)
    total = jnp.sum(weights, axis=-1, keepdims=True)
    output = jnp.dot(weights.astype(jnp.bfloat16), values, preferred_element_type=jnp.float32)
    return output / total, (highest + jnp.log2(total)) * LN2


def kernel(
    devices,
    held,
    most,
    group,
    slot_hbm,
    length_hbm,
    image_hbm,
    text_length_hbm,
    query_hbm,
    ikey_hbm,
    ivalue_hbm,
    tkey_hbm,
    tvalue_hbm,
    out_ref,
    slot_ref,
    length_ref,
    image_ref,
    text_length_ref,
    query_ref,
    ikey,
    ivalue,
    tkey,
    tvalue,
    send,
    recv,
    result,
    back,
    text_out,
    text_lse,
    lengths,
    local_sem,
    send_sem,
    recv_sem,
    result_sem,
    back_sem,
):
    me = lax.axis_index("seq")
    local_heads, rows, head_size = query_ref.shape
    local_kv = ikey.shape[1]
    image_tokens = ikey.shape[2]
    text_tokens = tkey.shape[2]
    images = slot_ref.shape[0]
    slots = images * most
    blocks = rows // BLOCK
    factor = LOG2E / math.sqrt(head_size)

    barrier = pltpu.get_barrier_semaphore()

    @pl.loop(1, devices)
    def _(step):
        pl.semaphore_signal(
            barrier, inc=1, device_id={"seq": partner(me, step, devices)}, device_id_type=MESH
        )

    copies = [
        pltpu.make_async_copy(source, target, local_sem.at[index])
        for index, (source, target) in enumerate(
            (
                (query_hbm, query_ref),
                (slot_hbm, slot_ref),
                (image_hbm, image_ref),
                (length_hbm, length_ref),
                (text_length_hbm, text_length_ref),
                (tkey_hbm, tkey),
                (tvalue_hbm, tvalue),
                (ikey_hbm, ikey),
                (ivalue_hbm, ivalue),
            )
        )
    ]
    for copy in copies:
        copy.start()
    loads = copies[5:]

    copies[1].wait()
    copies[2].wait()
    image = image_ref[...]
    slot = jnp.zeros_like(image)
    for index in range(images):
        place = slot_ref[index]
        place = partner(me, place // held, devices) * held + lax.rem(place, held)
        slot = jnp.where(image == index, place, slot)
    hits = slot == lax.broadcasted_iota(jnp.int32, (images, rows), 0)
    earlier = lax.broadcasted_iota(jnp.int32, (rows, rows), 0) < lax.broadcasted_iota(
        jnp.int32, (rows, rows), 1
    )
    counts = jnp.dot(
        hits.astype(jnp.float32).astype(jnp.bfloat16),
        earlier.astype(jnp.float32).astype(jnp.bfloat16),
        preferred_element_type=jnp.float32,
    )
    rank = jnp.sum(jnp.where(hits, counts, 0.0), axis=0, keepdims=True)
    target = slot.astype(jnp.float32) * most + rank
    dispatch = (
        lax.broadcasted_iota(jnp.int32, (slots, rows), 0).astype(jnp.float32) == target
    ).astype(jnp.float32).astype(jnp.bfloat16)
    copies[0].wait()
    for head in range(local_heads):
        moved = jnp.dot(dispatch, query_ref[head], preferred_element_type=jnp.float32)
        send[:, :, head] = moved.astype(jnp.bfloat16).reshape(devices, held, most, head_size)

    pl.semaphore_wait(barrier, devices - 1)

    def forward(step):
        return pltpu.make_async_remote_copy(
            src_ref=send.at[step],
            dst_ref=recv.at[step],
            send_sem=send_sem.at[step],
            recv_sem=recv_sem.at[step],
            device_id={"seq": partner(me, step, devices)},
            device_id_type=MESH,
        )

    def returning(step):
        return pltpu.make_async_remote_copy(
            src_ref=result.at[step],
            dst_ref=back.at[step],
            send_sem=result_sem.at[step],
            recv_sem=back_sem.at[step],
            device_id={"seq": partner(me, step, devices)},
            device_id_type=MESH,
        )

    @pl.loop(1, devices)
    def _(step):
        forward(step).start()

    copies[3].wait()
    copies[4].wait()
    lengths[...] = jnp.broadcast_to(
        text_length_ref[...].astype(jnp.float32), (rows, rows)
    ).T

    def place(lse, count):
        lane = lax.broadcasted_iota(jnp.int32, (count, head_size), 1)
        plane = jnp.zeros((count, head_size), jnp.float32)
        for head in range(local_heads):
            plane = jnp.where(lane == head, lse[head], plane)
        return plane

    loads[0].wait()
    loads[1].wait()

    def text(block):
        first = block * BLOCK
        first = first if isinstance(first, int) else pl.multiple_of(first, BLOCK)
        window = pl.ds(first, BLOCK)
        token = lax.broadcasted_iota(jnp.int32, (BLOCK, BLOCK * text_tokens), 1)
        offset = (
            token - text_tokens * lax.broadcasted_iota(jnp.int32, token.shape, 0)
        ).astype(jnp.float32)
        valid = (offset >= 0.0) & (offset < lengths[window, 0:1])
        bias = jnp.where(valid, 0.0, NEGATIVE)
        lses = []
        for kv in range(local_kv):
            query = query_ref[kv * group : (kv + 1) * group, window, :]
            query = query.reshape(group * BLOCK, head_size)
            keys = tkey[window, kv].reshape(BLOCK * text_tokens, head_size)
            values = tvalue[window, kv].reshape(BLOCK * text_tokens, head_size)

            def mask(scores):
                scores = scores.reshape(group, BLOCK, BLOCK * text_tokens) + bias[None]
                return scores.reshape(group * BLOCK, BLOCK * text_tokens)

            output, lse = attend(query, keys, values, mask, factor)
            text_out[kv * group : (kv + 1) * group, window, :] = output.reshape(
                group, BLOCK, head_size
            )
            lses += [lse[head * BLOCK : (head + 1) * BLOCK] for head in range(group)]
        text_lse[window, :] = place(lses, BLOCK)

    loads[2].wait()
    loads[3].wait()
    token = lax.broadcasted_iota(jnp.int32, (1, image_tokens), 1)
    biases = [jnp.where(token < length_ref[index], 0.0, NEGATIVE) for index in range(held)]

    def process(source, target):
        packed = jnp.zeros((most, head_size), jnp.float32)
        for index in range(held):
            lses = []
            for kv in range(local_kv):
                query = source[index, kv * group : (kv + 1) * group]
                query = query.reshape(group * most, head_size)
                output, lse = attend(
                    query,
                    ikey[index, kv],
                    ivalue[index, kv],
                    lambda scores: scores + biases[index],
                    factor,
                )
                start = index * local_heads + kv * group
                target[start : start + group] = output.astype(
                    jnp.bfloat16
                ).reshape(group, most, head_size)
                lses += [lse[head * most : (head + 1) * most] for head in range(group)]
            plane = place(lses, most)
            high = plane.astype(jnp.bfloat16).astype(jnp.float32)
            rest = plane - high
            middle = rest.astype(jnp.bfloat16).astype(jnp.float32)
            low = rest - middle
            for part, piece in enumerate((high, middle, low)):
                shift = LANES * (SPLIT * index + part)
                packed = packed + (pltpu.roll(piece, shift, 1) if shift else piece)
        target[held * local_heads] = packed.astype(jnp.bfloat16)

    for block in range(FIRST):
        text(block)
    process(send.at[0], back.at[0])

    @pl.loop(1, devices)
    def _(step):
        @pl.when(step + (FIRST - 1) < blocks)
        def _():
            text(step + (FIRST - 1))

        forward(step).wait_recv()
        process(recv.at[step], result.at[step])
        returning(step).start()

    for block in range(devices + FIRST - 1, blocks):
        text(block)

    sought = jnp.broadcast_to(target, (rows, rows)).T
    lane = lax.broadcasted_iota(jnp.int32, (rows, rows), 1).astype(jnp.float32)
    combine = jnp.concatenate(
        [
            (sought == lane + float(start)).astype(jnp.float32).astype(jnp.bfloat16)
            for start in range(0, slots, rows)
        ],
        axis=1,
    )

    @pl.loop(1, devices)
    def _(step):
        forward(step).wait_send()
        returning(step).wait_send()
        returning(step).wait_recv()

    planes = back[:, held * local_heads].reshape(devices, 1, most, head_size)
    spread = jnp.broadcast_to(planes, (devices, held, most, head_size)).reshape(slots, head_size)
    at_lane = lax.broadcasted_iota(jnp.int32, (1, 1, 1, head_size), 3)
    at_held = lax.broadcasted_iota(jnp.int32, (1, held, 1, 1), 1)
    low_lane = at_held * (SPLIT * LANES)
    own_lanes = (at_lane >= low_lane) & (at_lane < low_lane + SPLIT * LANES)
    own_lanes = jnp.broadcast_to(
        own_lanes.astype(jnp.float32), (devices, held, most, head_size)
    ).reshape(slots, head_size).astype(jnp.bfloat16)
    parts = jnp.dot(combine, spread * own_lanes, preferred_element_type=jnp.float32)
    image_lse = parts
    for piece in range(1, SPLIT * held):
        image_lse = image_lse + pltpu.roll(parts, head_size - LANES * piece, 1)
    own_lse = text_lse[...]
    upper = jnp.maximum(image_lse, own_lse)
    image_weight = jnp.exp(image_lse - upper)
    text_weight = jnp.exp(own_lse - upper)
    whole = image_weight + text_weight
    image_weight = image_weight / whole
    text_weight = text_weight / whole
    def gathered(head):
        pieces = [back[:, index * local_heads + head] for index in range(held)]
        return jnp.stack(pieces, axis=1).reshape(slots, head_size)

    for head in range(local_heads):
        image_part = jnp.dot(
            combine,
            gathered(head),
            preferred_element_type=jnp.float32,
        )
        merged = (
            image_weight[:, head : head + 1] * image_part
            + text_weight[:, head : head + 1] * text_out[head]
        )
        out_ref[head] = merged.astype(jnp.bfloat16)


def spread_planes(planes, held):
    units, _, head_size = planes.shape
    planes = planes.reshape(units, 1, BLOCK, head_size)
    spread = jnp.broadcast_to(planes, (units, held, BLOCK, head_size))
    at_lane = lax.broadcasted_iota(jnp.int32, (1, 1, 1, head_size), 3)
    at_held = lax.broadcasted_iota(jnp.int32, (1, held, 1, 1), 1)
    low_lane = at_held * (SPLIT * LANES)
    own_lanes = (at_lane >= low_lane) & (at_lane < low_lane + SPLIT * LANES)
    own_lanes = jnp.broadcast_to(own_lanes.astype(jnp.float32), spread.shape)
    own_lanes = own_lanes.reshape(-1, head_size).astype(jnp.bfloat16)
    return spread.reshape(-1, head_size) * own_lanes


def place(lse, count, head_size):
    lane = lax.broadcasted_iota(jnp.int32, (count, head_size), 1)
    plane = jnp.zeros((count, head_size), jnp.float32)
    for head, column in enumerate(lse):
        plane = jnp.where(lane == head, column, plane)
    return plane


def one_hot(condition):
    return condition.astype(jnp.float32).astype(jnp.bfloat16)


def cross_lanes(left, right):
    return lax.dot_general(
        left, right, (((1,), (1,)), ((), ())), preferred_element_type=jnp.float32
    )


LOCAL = 4
OWN, NEAR, OVER, BASE = 0, (0, 1, 2, 7), (3, 5), (4, 6)
UNITS = 8
BLOCKS = (*NEAR, *BASE)
EARLY = 3


def fast_kernel(
    devices,
    replicas,
    held,
    group,
    spare,
    slot_hbm,
    length_hbm,
    image_hbm,
    text_length_hbm,
    query_hbm,
    ikey_hbm,
    ivalue_hbm,
    tkey_hbm,
    tvalue_hbm,
    out_ref,
    flag_ref,
    slot_ref,
    length_ref,
    image_ref,
    text_length_ref,
    query_ref,
    ikey,
    ivalue,
    tkey,
    tvalue,
    send,
    recv,
    result,
    back,
    fan,
    ret,
    bundle_send,
    bundle_recv,
    bundle_result,
    bundle_back,
    metas,
    group_send,
    group_recv,
    text_out,
    text_lse,
    lengths,
    local_sem,
    send_sem,
    recv_sem,
    result_sem,
    back_sem,
    fan_sem,
    fan_recv_sem,
    ret_sem,
    ret_recv_sem,
    bundle_sem,
    meta_sem,
    meta_recv_sem,
    group_sem,
    group_recv_sem,
):
    me = lax.axis_index("seq")
    replica = lax.axis_index("groups")
    local_heads, rows, head_size = query_ref.shape
    local_kv = ikey.shape[1]
    image_tokens = ikey.shape[2]
    text_tokens = tkey.shape[2]
    images = slot_ref.shape[0]
    half = BLOCK // 2
    near = LOCAL * held
    text_blocks = rows // BLOCK
    factor = LOG2E / math.sqrt(head_size)

    barrier = pltpu.get_barrier_semaphore()

    @pl.loop(1, devices)
    def _(step):
        pl.semaphore_signal(
            barrier, inc=1, device_id={"seq": partner(me, step, devices)}, device_id_type=MESH
        )

    for turn in range(1, replicas):
        pl.semaphore_signal(
            barrier,
            inc=1,
            device_id={"groups": lax.rem(replica + turn, replicas)},
            device_id_type=MESH,
        )

    copies = [
        pltpu.make_async_copy(source, target, local_sem.at[index])
        for index, (source, target) in enumerate(
            (
                (query_hbm, query_ref),
                (slot_hbm, slot_ref),
                (image_hbm, image_ref),
                (length_hbm, length_ref),
                (text_length_hbm, text_length_ref),
                (tkey_hbm, tkey),
                (tvalue_hbm, tvalue),
                (ikey_hbm, ikey),
                (ivalue_hbm, ivalue),
            )
        )
    ]
    for copy in copies:
        copy.start()
    loads = copies[5:]

    copies[1].wait()
    copies[2].wait()

    earlier = one_hot(
        lax.broadcasted_iota(jnp.int32, (rows, rows), 0)
        < lax.broadcasted_iota(jnp.int32, (rows, rows), 1)
    )

    def route(image, origin):
        step = jnp.zeros(image.shape, jnp.float32)
        index = jnp.zeros(image.shape, jnp.float32)
        spot = jnp.zeros(image.shape, jnp.int32)
        for name in range(images):
            slot = slot_ref[name]
            owner = partner(origin, slot // held, devices)
            which = lax.rem(slot, held)
            step = jnp.where(image == name, owner.astype(jnp.float32), step)
            index = jnp.where(image == name, which.astype(jnp.float32), index)
            spot = jnp.where(image == name, slot, spot)
        hits = spot == lax.broadcasted_iota(jnp.int32, (images, rows), 0)
        counts = jnp.dot(one_hot(hits), earlier, preferred_element_type=jnp.float32)
        rank = jnp.sum(jnp.where(hits, counts, 0.0), axis=0, keepdims=True)
        over = (step >= LOCAL) & (rank >= half)
        over = jnp.where(over, 1.0, 0.0)
        order = jnp.dot(
            jnp.broadcast_to(over, (BLOCK, rows)).astype(jnp.bfloat16),
            earlier,
            preferred_element_type=jnp.float32,
        )[0:1]
        return step, index, rank, over > 0.0, order

    def paired(step, index, rank):
        pair = jnp.where(step >= 2.0, 1.0, 0.0)
        parity = step - 2.0 * pair
        return (pair * held + index) * BLOCK + parity * half + rank

    step, index, rank, over, order = route(image_ref[...], me)
    target = jnp.where(
        step < LOCAL,
        (step * held + index) * BLOCK + rank,
        jnp.where(
            over,
            (LOCAL + 2.0) * held * BLOCK + order,
            LOCAL * held * BLOCK + paired(step - LOCAL, index, rank),
        ),
    )
    places = (LOCAL + 2) * held * BLOCK + spare
    dispatch = one_hot(
        lax.broadcasted_iota(jnp.int32, (places, rows), 0).astype(jnp.float32) == target
    )
    copies[0].wait()
    for head in range(local_heads):
        moved = jnp.dot(dispatch, query_ref[head], preferred_element_type=jnp.float32)
        moved = moved.astype(jnp.bfloat16)
        blocks = moved[: (LOCAL + 2) * held * BLOCK].reshape(-1, held, BLOCK, head_size)
        recv[OWN, :, head] = blocks[0]
        send[:, :, head] = blocks[1:]
        bundle_send[head] = moved[(LOCAL + 2) * held * BLOCK :]

    pl.semaphore_wait(barrier, devices - 1 + replicas - 1)

    def remote(source, sink, source_sem, sink_sem, step):
        return pltpu.make_async_remote_copy(
            src_ref=source,
            dst_ref=sink,
            send_sem=source_sem,
            recv_sem=sink_sem,
            device_id={"seq": partner(me, step, devices)},
            device_id_type=MESH,
        )

    def meta(step):
        return remote(image_ref, metas.at[step], meta_sem.at[step], meta_recv_sem.at[step], step)

    def bundle_out():
        return remote(bundle_send, bundle_recv, bundle_sem.at[0], bundle_sem.at[1], LOCAL)

    def bundle_home():
        return remote(bundle_result, bundle_back, bundle_sem.at[2], bundle_sem.at[3], LOCAL)

    def part(parity):
        return pl.ds(parity * half, half)

    def forward(step):
        if step < LOCAL:
            source, sink = send.at[step - 1], recv.at[NEAR[step]]
        else:
            pair, parity = divmod(step - LOCAL, 2)
            source = send.at[LOCAL - 1 + pair, :, :, part(parity)]
            sink = recv.at[BASE[pair], :, :, part(parity)]
        return remote(source, sink, send_sem.at[step], recv_sem.at[step], step)

    def returning(step):
        if step < LOCAL:
            source, sink = result.at[NEAR[step]], back.at[NEAR[step]]
        else:
            pair, parity = divmod(step - LOCAL, 2)
            source = result.at[BASE[pair], :, part(parity)]
            sink = back.at[BASE[pair], :, part(parity)]
        return remote(source, sink, result_sem.at[step], back_sem.at[step], step)

    def fan_out(step):
        pair, parity = divmod(step, 2)
        source = fan.at[pair, :, :, part(parity)]
        sink = recv.at[OVER[pair], :, :, part(parity)]
        return remote(source, sink, fan_sem.at[step], fan_recv_sem.at[step], step)

    def fan_home(step):
        pair, parity = divmod(step, 2)
        source = result.at[OVER[pair], :, part(parity)]
        sink = ret.at[pair, :, part(parity)]
        return remote(source, sink, ret_sem.at[step], ret_recv_sem.at[step], step)

    @pl.loop(1, devices)
    def _(step):
        meta(step).start()

    bundle_out().start()
    for step in range(1, devices):
        forward(step).start()

    copies[3].wait()
    copies[4].wait()
    lengths[...] = jnp.broadcast_to(
        text_length_ref[...].astype(jnp.float32), (rows, rows)
    ).T

    loads[0].wait()
    loads[1].wait()

    def text(block):
        window = pl.ds(pl.multiple_of(block * BLOCK, BLOCK), BLOCK)
        token = lax.broadcasted_iota(jnp.int32, (BLOCK, BLOCK * text_tokens), 1)
        offset = (
            token - text_tokens * lax.broadcasted_iota(jnp.int32, token.shape, 0)
        ).astype(jnp.float32)
        valid = (offset >= 0.0) & (offset < lengths[window, 0:1])
        bias = jnp.where(valid, 0.0, NEGATIVE)
        lses = []
        for kv in range(local_kv):
            query = query_ref[kv * group : (kv + 1) * group, window, :]
            query = query.reshape(group * BLOCK, head_size)
            keys = tkey[window, kv].reshape(BLOCK * text_tokens, head_size)
            values = tvalue[window, kv].reshape(BLOCK * text_tokens, head_size)

            def mask(scores):
                scores = scores.reshape(group, BLOCK, BLOCK * text_tokens) + bias[None]
                return scores.reshape(group * BLOCK, BLOCK * text_tokens)

            output, lse = attend(query, keys, values, mask, factor)
            text_out[kv * group : (kv + 1) * group, window, :] = output.reshape(
                group, BLOCK, head_size
            )
            lses += [lse[head * BLOCK : (head + 1) * BLOCK] for head in range(group)]
        text_lse[window, :] = place(lses, BLOCK, head_size)

    @pl.loop(0, EARLY)
    def _(block):
        text(block)

    loads[2].wait()
    loads[3].wait()
    token = lax.broadcasted_iota(jnp.int32, (1, image_tokens), 1)
    biases = [jnp.where(token < length_ref[index], 0.0, NEGATIVE) for index in range(held)]

    def process(source, sink):
        packed = jnp.zeros((BLOCK, head_size), jnp.float32)
        for index in range(held):
            lses = []
            for kv in range(local_kv):
                query = source[index, kv * group : (kv + 1) * group]
                query = query.reshape(group * BLOCK, head_size)
                output, lse = attend(
                    query,
                    ikey[index, kv],
                    ivalue[index, kv],
                    lambda scores: scores + biases[index],
                    factor,
                )
                start = index * local_heads + kv * group
                sink[start : start + group] = output.astype(jnp.bfloat16).reshape(
                    group, BLOCK, head_size
                )
                lses += [lse[head * BLOCK : (head + 1) * BLOCK] for head in range(group)]
            plane = place(lses, BLOCK, head_size)
            high = plane.astype(jnp.bfloat16).astype(jnp.float32)
            rest = plane - high
            middle = rest.astype(jnp.bfloat16).astype(jnp.float32)
            low = rest - middle
            for number, piece in enumerate((high, middle, low)):
                shift = LANES * (SPLIT * index + number)
                packed = packed + (pltpu.roll(piece, shift, 1) if shift else piece)
        sink[held * local_heads] = packed.astype(jnp.bfloat16)

    def relay_places():
        other = partner(me, LOCAL, devices)
        step, index, rank, over, order = route(metas[LOCAL], other)
        spot = jnp.where(over, paired(step - LOCAL, index, rank - half), -1.0)
        order = jnp.where(over, order, -1.0)
        spots = LOCAL * held * half
        spot = one_hot(
            lax.broadcasted_iota(jnp.int32, (spots, rows), 0).astype(jnp.float32) == spot
        )
        order = one_hot(
            lax.broadcasted_iota(jnp.int32, (spare, rows), 0).astype(jnp.float32) == order
        )
        return spot, order

    def relay():
        bundle_out().wait_recv()
        spot, order = relay_places()
        scatter = cross_lanes(spot, order).astype(jnp.bfloat16)
        for head in range(local_heads):
            moved = jnp.dot(scatter, bundle_recv[head], preferred_element_type=jnp.float32)
            moved = moved.astype(jnp.bfloat16).reshape(2, held, BLOCK, head_size)
            fan[:, :, head] = moved
            recv[OVER[0], :, head, 0:half] = moved[0, :, 0:half]
        for step in range(1, LOCAL):
            fan_out(step).start()

    def collect():
        for step in range(1, LOCAL):
            fan_home(step).wait_recv()
        spot, order = relay_places()
        gather = cross_lanes(order, spot).astype(jnp.bfloat16)
        upper = lax.broadcasted_iota(jnp.int32, (BLOCK, head_size), 0) < half

        def tile(pair, number):
            if pair:
                return ret[pair, number]
            own = result[OVER[0], number].astype(jnp.float32)
            return jnp.where(upper, own, ret[0, number].astype(jnp.float32)).astype(jnp.bfloat16)

        for head in range(local_heads):
            pieces = [
                tile(pair, which * local_heads + head) for pair in range(2) for which in range(held)
            ]
            moved = jnp.dot(
                gather, jnp.concatenate(pieces, axis=0), preferred_element_type=jnp.float32
            )
            bundle_result[head] = moved.astype(jnp.bfloat16)
        planes = jnp.stack([tile(pair, held * local_heads) for pair in range(2)], axis=0)
        moved = jnp.dot(gather, spread_planes(planes, held), preferred_element_type=jnp.float32)
        bundle_result[local_heads] = moved.astype(jnp.bfloat16)
        bundle_home().start()

    def judge():
        @pl.loop(1, devices)
        def _(step):
            meta(step).wait_recv()

        mine = lax.rem(me // LOCAL, 2)
        named = jnp.concatenate(
            [image_ref[...]] + [metas[step] for step in range(1, devices)], axis=0
        )
        side = lax.broadcasted_iota(jnp.int32, (devices, 1), 0) >= LOCAL
        total = jnp.zeros((devices, 1), jnp.float32)
        for name in range(images):
            there = lax.rem(slot_ref[name] // held // LOCAL, 2)
            apart = (mine + there - 2 * mine * there).astype(jnp.float32)
            count = jnp.sum(jnp.where(named == name, 1.0, 0.0), axis=1, keepdims=True)
            excess = jnp.maximum(count - half, 0.0)
            total = total + excess * jnp.where(side, 1.0 - apart, apart)
        full = jnp.where(total > spare, 1.0, 0.0)
        full = jnp.max(full, axis=0, keepdims=True)
        group_send[...] = jnp.broadcast_to(full, (1, rows)).astype(jnp.int32)

    def tell(turn):
        return pltpu.make_async_remote_copy(
            src_ref=group_send,
            dst_ref=group_recv.at[turn - 1],
            send_sem=group_sem.at[turn - 1],
            recv_sem=group_recv_sem.at[turn - 1],
            device_id={"groups": lax.rem(replica + turn, replicas)},
            device_id_type=MESH,
        )

    judge()
    for turn in range(1, replicas):
        tell(turn).start()

    @pl.loop(0, UNITS)
    def _(unit):
        for step in range(1, LOCAL):
            @pl.when(unit == NEAR[step])
            def _():
                forward(step).wait_recv()

        for pair in range(2):
            @pl.when(unit == OVER[pair])
            def _():
                for step in range(max(1, 2 * pair), 2 * pair + 2):
                    fan_out(step).wait_recv()

            @pl.when(unit == BASE[pair])
            def _():
                for step in (LOCAL + 2 * pair, LOCAL + 2 * pair + 1):
                    forward(step).wait_recv()

        process(recv.at[unit], result.at[unit])

        @pl.when(unit == OWN)
        def _():
            relay()

        for step in range(1, LOCAL):
            @pl.when(unit == NEAR[step])
            def _():
                returning(step).start()

        for pair in range(2):
            @pl.when(unit == OVER[pair])
            def _():
                for step in range(max(1, 2 * pair), 2 * pair + 2):
                    fan_home(step).start()

            @pl.when(unit == BASE[pair])
            def _():
                for step in (LOCAL + 2 * pair, LOCAL + 2 * pair + 1):
                    returning(step).start()

        @pl.when(unit == BASE[1])
        def _():
            collect()

    @pl.loop(EARLY, text_blocks)
    def _(block):
        text(block)

    sought = jnp.broadcast_to(target, (rows, rows)).T
    lane = lax.broadcasted_iota(jnp.int32, (rows, rows), 1).astype(jnp.float32)
    local_rows = LOCAL * held * BLOCK
    cross_rows = places - local_rows
    from_near = one_hot(sought == lane)
    from_far = one_hot(sought == lane + float(local_rows))[:, :cross_rows]

    for turn in range(1, replicas):
        tell(turn).wait()
    full = jnp.max(group_send[...].astype(jnp.float32))
    for turn in range(1, replicas):
        full = jnp.maximum(full, jnp.max(group_recv[turn - 1].astype(jnp.float32)))
    flag_ref[0] = full.astype(jnp.int32)

    @pl.loop(1, devices)
    def _(step):
        meta(step).wait_send()

    bundle_out().wait_send()
    for step in range(1, LOCAL):
        fan_out(step).wait_send()
        fan_home(step).wait_send()
    bundle_home().wait()
    for step in range(1, devices):
        forward(step).wait_send()
        returning(step).wait()

    def block_of(number, rows_of):
        return (result if number == OWN else back)[number, rows_of]

    planes = jnp.stack([block_of(number, held * local_heads) for number in BLOCKS], axis=0)
    spread = spread_planes(planes, held)
    parts = jnp.dot(from_near, spread[:local_rows], preferred_element_type=jnp.float32)
    parts = parts + jnp.dot(
        from_far,
        jnp.concatenate([spread[local_rows:], bundle_back[local_heads]], axis=0),
        preferred_element_type=jnp.float32,
    )
    image_lse = parts
    for piece in range(1, SPLIT * held):
        image_lse = image_lse + pltpu.roll(parts, head_size - LANES * piece, 1)
    own_lse = text_lse[...]
    upper = jnp.maximum(image_lse, own_lse)
    image_weight = jnp.exp(image_lse - upper)
    text_weight = jnp.exp(own_lse - upper)
    whole = image_weight + text_weight
    image_weight = image_weight / whole
    text_weight = text_weight / whole

    for head in range(local_heads):
        pieces = [
            block_of(number, which * local_heads + head)
            for number in BLOCKS
            for which in range(held)
        ]
        middle = LOCAL * held
        image_part = jnp.dot(
            from_near,
            jnp.concatenate(pieces[:middle], axis=0),
            preferred_element_type=jnp.float32,
        ) + jnp.dot(
            from_far,
            jnp.concatenate(pieces[middle:] + [bundle_back[head]], axis=0),
            preferred_element_type=jnp.float32,
        )
        merged = (
            image_weight[:, head : head + 1] * image_part
            + text_weight[:, head : head + 1] * text_out[head]
        )
        out_ref[head] = merged.astype(jnp.bfloat16)


def on_device(
    queries,
    request_image,
    image_slot,
    image_lengths,
    image_keys,
    image_values,
    text_keys,
    text_values,
    text_lengths,
):
    rows, local_heads, head_size = queries.shape
    held, local_kv, image_tokens, _ = image_keys.shape
    text_tokens = text_keys.shape[2]
    group = local_heads // local_kv
    images = image_slot.shape[0]
    devices = lax.axis_size("seq")
    most = -(-max(2, 2 * rows // images) // BLOCK) * BLOCK
    hbm = pl.BlockSpec(memory_space=pltpu.HBM)
    operands = [
        pltpu.with_memory_space_constraint(operand, pltpu.HBM)
        for operand in (
            image_slot,
            image_lengths,
            request_image.reshape(1, rows),
            text_lengths.reshape(1, rows),
            jnp.transpose(queries, (1, 0, 2)),
            image_keys,
            image_values,
            text_keys,
            text_values,
        )
    ]
    outcome = pltpu.VMEM((local_heads, rows, head_size), jnp.bfloat16)
    common = [
        pltpu.SMEM(image_slot.shape, jnp.int32),
        pltpu.SMEM(image_lengths.shape, jnp.int32),
        pltpu.VMEM((1, rows), jnp.int32),
        pltpu.VMEM((1, rows), jnp.int32),
        pltpu.VMEM((local_heads, rows, head_size), jnp.bfloat16),
        pltpu.VMEM(image_keys.shape, jnp.bfloat16),
        pltpu.VMEM(image_values.shape, jnp.bfloat16),
        pltpu.VMEM(text_keys.shape, jnp.bfloat16),
        pltpu.VMEM(text_values.shape, jnp.bfloat16),
    ]
    texts = [
        pltpu.VMEM((local_heads, rows, head_size), jnp.float32),
        pltpu.VMEM((rows, head_size), jnp.float32),
        pltpu.VMEM((rows, rows), jnp.float32),
        pltpu.SemaphoreType.DMA((9,)),
    ]
    results = held * local_heads + 1

    def plain(identity):
        return pl.pallas_call(
            functools.partial(kernel, devices, held, most, group),
            out_shape=outcome,
            in_specs=[hbm] * 9,
            out_specs=pl.BlockSpec(memory_space=pltpu.VMEM),
            scratch_shapes=common
            + [
                pltpu.VMEM((devices, held, local_heads, most, head_size), jnp.bfloat16),
                pltpu.VMEM((devices, held, local_heads, most, head_size), jnp.bfloat16),
                pltpu.VMEM((devices, results, most, head_size), jnp.bfloat16),
                pltpu.VMEM((devices, results, most, head_size), jnp.bfloat16),
            ]
            + texts
            + [pltpu.SemaphoreType.DMA((devices,))] * 4,
            compiler_params=pltpu.CompilerParams(
                collective_id=identity, has_side_effects=True, vmem_limit_bytes=LIMIT
            ),
        )(*operands)

    if devices != 2 * LOCAL or most != BLOCK or 2 * rows // images <= BLOCK // 2:
        return jnp.transpose(plain(0), (1, 0, 2))

    replicas = lax.axis_size("groups")
    spare = rows // 4
    half = BLOCK // 2
    moved, flag = pl.pallas_call(
        functools.partial(fast_kernel, devices, replicas, held, group, spare),
        out_shape=(outcome, pltpu.SMEM((1,), jnp.int32)),
        in_specs=[hbm] * 9,
        out_specs=(
            pl.BlockSpec(memory_space=pltpu.VMEM),
            pl.BlockSpec(memory_space=pltpu.SMEM),
        ),
        scratch_shapes=common
        + [
            pltpu.VMEM((LOCAL + 1, held, local_heads, BLOCK, head_size), jnp.bfloat16),
            pltpu.VMEM((UNITS, held, local_heads, BLOCK, head_size), jnp.bfloat16),
            pltpu.VMEM((UNITS, results, BLOCK, head_size), jnp.bfloat16),
            pltpu.VMEM((UNITS, results, BLOCK, head_size), jnp.bfloat16),
            pltpu.VMEM((2, held, local_heads, BLOCK, head_size), jnp.bfloat16),
            pltpu.VMEM((2, results, BLOCK, head_size), jnp.bfloat16),
            pltpu.VMEM((local_heads, spare, head_size), jnp.bfloat16),
            pltpu.VMEM((local_heads, spare, head_size), jnp.bfloat16),
            pltpu.VMEM((local_heads + 1, spare, head_size), jnp.bfloat16),
            pltpu.VMEM((local_heads + 1, spare, head_size), jnp.bfloat16),
            pltpu.VMEM((devices, 1, rows), jnp.int32),
            pltpu.VMEM((1, rows), jnp.int32),
            pltpu.VMEM((max(1, replicas - 1), 1, rows), jnp.int32),
        ]
        + texts
        + [pltpu.SemaphoreType.DMA((devices,))] * 4
        + [pltpu.SemaphoreType.DMA((LOCAL,))] * 5
        + [pltpu.SemaphoreType.DMA((devices,))] * 2
        + [pltpu.SemaphoreType.DMA((max(1, replicas - 1),))] * 2,
        compiler_params=pltpu.CompilerParams(
            collective_id=0, has_side_effects=True, vmem_limit_bytes=LIMIT
        ),
    )(*operands)
    moved = lax.cond(flag[0] > 0, lambda: plain(1), lambda: moved)
    return jnp.transpose(moved, (1, 0, 2))


def solution(mesh):
    in_specs = (
        P(("groups", "seq"), "head", None),
        P(("groups", "seq"), None),
        P("groups"),
        P(("groups", "seq")),
        P(("groups", "seq"), "head", None, None),
        P(("groups", "seq"), "head", None, None),
        P(("groups", "seq"), "head", None, None),
        P(("groups", "seq"), "head", None, None),
        P(("groups", "seq")),
    )
    out_specs = P(("groups", "seq"), "head", None)
    return jax.shard_map(
        on_device, mesh=mesh, in_specs=in_specs, out_specs=out_specs, check_vma=False
    )
```
